32 devices in a mesh: rep: 8 (over z, core), tp: 4 (over y, x).
Axes of the slice: x: 2, y: 2, z: 4, core: 2. Of those that a mesh axis runs over, the one named last changes fastest.
Arguments:
- delta_query: bfloat16 [8, 2, 2048, 3072], P('rep', None, None, 'tp'), may hold values from -6 to 6
- master_query: float32 [2, 2048, 3072], P(None, 'rep', 'tp'), may hold values from -3 to 3
- moment_query: float32 [2, 2048, 3072], P(None, 'rep', 'tp'), may hold values from -3 to 3
- delta_latent: bfloat16 [8, 2, 512, 4096], P('rep', None, None, 'tp'), may hold values from -6 to 6
- master_latent: float32 [2, 512, 4096], P(None, 'rep', 'tp'), may hold values from -3 to 3
- moment_latent: float32 [2, 512, 4096], P(None, 'rep', 'tp'), may hold values from -3 to 3
- delta_output: bfloat16 [8, 2, 2048, 2048], P('rep', None, 'tp'), may hold values from -6 to 6
- master_output: float32 [2, 2048, 2048], P(None, 'tp', 'rep'), may hold values from -3 to 3
- moment_output: float32 [2, 2048, 2048], P(None, 'tp', 'rep'), may hold values from -3 to 3
Outputs:
- params_query: bfloat16 [2, 2048, 3072], P(None, None, 'tp')
- new_master_query: float32 [2, 2048, 3072], P(None, 'rep', 'tp')
- new_moment_query: float32 [2, 2048, 3072], P(None, 'rep', 'tp')
- params_latent: bfloat16 [2, 512, 4096], P(None, None, 'tp')
- new_master_latent: float32 [2, 512, 4096], P(None, 'rep', 'tp')
- new_moment_latent: float32 [2, 512, 4096], P(None, 'rep', 'tp')
- params_output: bfloat16 [2, 2048, 2048], P(None, 'tp')
- new_master_output: float32 [2, 2048, 2048], P(None, 'tp', 'rep')
- new_moment_output: float32 [2, 2048, 2048], P(None, 'tp', 'rep')
The draws below stay inside these ranges and needn't reach their ends.
All inputs are finite; a program needn't handle non-finite values.
Results may differ from the reference program's by a relative error of at most 0.012.
Values may be sent and summed in bfloat16 or wider, within the bound.
A program may use at most 128 MiB of HBM per device.

```python
import jax
import jax.numpy as jnp
from jax import lax

D = 2048
KV_RANK = 512
LAYERS = 2
REPLICAS = 8
QCOLS = 3072
KVCOLS = 4096
OROWS = 2048


def spiked(drawn, rng, source, target, blocks, factor):
    owner, partner = [(jnp.arange(drawn.shape[dim]) // (drawn.shape[dim] // blocks)).reshape([-1 if axis == dim else 1 for axis in range(drawn.ndim)]) for dim in (source, target)]
    chosen = jax.random.permutation(rng, blocks)[partner]
    strong = (owner == chosen) | (owner == (partner + blocks // 2) % blocks)
    return jnp.where(strong, factor * drawn, drawn)


def level_of(own_key, dims, pieces, smallest, top_value):
    loudness = 1.0
    for dim, parts in pieces:
        steps = jax.random.uniform(jax.random.fold_in(jax.random.fold_in(own_key, 6), dim), (parts,), jnp.float32, smallest / len(pieces), top_value / len(pieces))
        loudness = loudness * jnp.repeat(jnp.exp(steps), dims[dim] // parts).reshape((-1,) + (1,) * (len(dims) - 1 - dim))
    return loudness


def gaussian(own_key, extent, scale, bound, shards=(), kind=jnp.bfloat16):
    drawn = jax.random.normal(own_key, extent, jnp.float32) * scale
    if len(shards) > 0:
        drawn = level_of(own_key, extent, shards, -0.22, 0.18) * drawn
    return jnp.clip(drawn, min=-bound, max=bound).astype(kind)


def noise_with(rng, dims, deviation, limit, shards, heavy, held_as=jnp.bfloat16):
    entries = deviation * jax.random.normal(rng, dims, jnp.float32)
    if shards:
        entries = entries * level_of(rng, dims, shards, -0.22, 0.18)
    return jnp.clip(spiked(entries, jax.random.fold_in(rng, 3), *heavy), -limit, limit).astype(held_as)


def setup_inputs(seed: int = 0) -> dict:
    streams_of = jax.random.split(jax.random.key(seed), 10)
    delta_query = noise_with(streams_of[0], (REPLICAS, LAYERS, D, QCOLS), 1.0, 6.0, ((0, 8), (3, 4)), (0, 2, 8, 2.0))
    master_query = gaussian(streams_of[1], (LAYERS, D, QCOLS), 0.5, 3.0, ((1, 8), (2, 4)), jnp.float32)
    moment_query = gaussian(streams_of[2], (LAYERS, D, QCOLS), 0.3, 3.0, ((1, 8), (2, 4)), jnp.float32)
    delta_latent = noise_with(streams_of[3], (REPLICAS, LAYERS, KV_RANK, KVCOLS), 1.0, 6.0, ((0, 8), (3, 4)), (0, 2, 8, 2.0))
    master_latent = gaussian(streams_of[4], (LAYERS, KV_RANK, KVCOLS), 0.5, 3.0, ((1, 8), (2, 4)), jnp.float32)
    moment_latent = gaussian(streams_of[5], (LAYERS, KV_RANK, KVCOLS), 0.3, 3.0, ((1, 8), (2, 4)), jnp.float32)
    delta_output = noise_with(streams_of[6], (REPLICAS, LAYERS, OROWS, D), 1.0, 6.0, ((0, 8), (2, 4)), (0, 3, 8, 2.0))
    master_output = gaussian(streams_of[7], (LAYERS, OROWS, D), 0.5, 3.0, ((1, 4), (2, 8)), jnp.float32)
    moment_output = gaussian(streams_of[8], (LAYERS, OROWS, D), 0.3, 3.0, ((1, 4), (2, 8)), jnp.float32)
    return dict(delta_query=delta_query, master_query=master_query, moment_query=moment_query, delta_latent=delta_latent, master_latent=master_latent, moment_latent=moment_latent, delta_output=delta_output, master_output=master_output, moment_output=moment_output)


OUTER_RATE = 0.7
OUTER_MOMENTUM = 0.9


def accumulate(delta):
    def add_replica(replica, running):
        return running + delta[replica].astype(jnp.float32)

    return lax.fori_loop(0, REPLICAS, add_replica, jnp.zeros(delta.shape[1:], jnp.float32))


def update(delta, master, moment):
    average = accumulate(delta) / REPLICAS
    momentum = OUTER_MOMENTUM * moment + average
    updated = master - OUTER_RATE * (average + OUTER_MOMENTUM * momentum)
    return updated.astype(jnp.bfloat16), updated, momentum


def reference(delta_query, master_query, moment_query, delta_latent, master_latent, moment_latent, delta_output, master_output, moment_output):
    query_params, query_master, query_moment = update(delta_query, master_query, moment_query)
    latent_params, latent_master, latent_moment = update(delta_latent, master_latent, moment_latent)
    output_params, output_master, output_moment = update(delta_output, master_output, moment_output)
    return (query_params, query_master, query_moment, latent_params, latent_master, latent_moment, output_params, output_master, output_moment)
```

```python
import functools

import jax
import jax.numpy as jnp
from jax import lax
from jax.experimental import pallas as pl
from jax.experimental.pallas import tpu as pltpu
from jax.sharding import PartitionSpec as P

OUTER_RATE = 0.7
OUTER_MOMENTUM = 0.9
MESH = pl.DeviceIdType.MESH
PIECES = 16
LEAD = 3


def plan(shapes, pieces):
    cuts = []
    for layers, rows, cols in shapes:
        if pieces % layers:
            return None
        per_layer = pieces // layers
        by_row = per_layer
        while by_row > 1 and (rows % by_row or (rows // by_row) % 16):
            by_row //= 2
        by_col = per_layer // by_row
        if by_row * by_col != per_layer or cols % by_col or (cols // by_col) % 128:
            return None
        cuts.append((per_layer, by_col, rows // by_row, cols // by_col))
    return cuts


def kernel(n, cuts, width, own_shapes, *refs):
    deltas, masters, moments = refs[0:9:3], refs[1:9:3], refs[2:9:3]
    params, new_masters, new_moments = refs[9:18:3], refs[10:18:3], refs[11:18:3]
    (theirs, mine, up_in, down_in, gathered, master, moment) = refs[18:25]
    (theirs_sem, mine_sem, up_sem, down_sem, gather_sem, state_sem,
     gather_up_sem, gather_down_sem, total_sem) = refs[25:]
    m = n // 2
    pieces = theirs.shape[0]
    me = lax.axis_index("rep")
    z, core = me // 2, me % 2
    partner = z * 2 + 1 - core
    above, below = (z + 1) * 2 + core, (z - 1) * 2 + core
    first, last = z == 0, z == m - 1

    def blocks(k):
        found, at = [], 0
        for a, (per_layer, by_col, rows, cols) in enumerate(cuts):
            layer, part = k // per_layer, k % per_layer
            row, col = (part // by_col) * rows, (part % by_col) * cols
            for b in range(cols // width):
                found.append((a, layer, row, rows, col + b * width, at))
                at += rows
        return found

    def whole_slice(a, layer, row, rows, col, owner):
        own_rows, own_cols = own_shapes[a][1:]
        if a < 2:
            row = row + owner * own_rows
        else:
            col = col + owner * own_cols
        return (layer, pl.ds(pl.multiple_of(row, 16), rows), pl.ds(pl.multiple_of(col, 128), width))

    def own_slice(a, layer, row, rows, col):
        return (layer, pl.ds(pl.multiple_of(row, 16), rows), pl.ds(pl.multiple_of(col, 128), width))

    def remote(src, dst, send, recv, rank):
        return pltpu.make_async_remote_copy(
            src_ref=src, dst_ref=dst, send_sem=send, recv_sem=recv,
            device_id={"rep": rank}, device_id_type=MESH,
        )

    def wait_bytes(ref, sem):
        pltpu.make_async_copy(ref, ref, sem).wait()

    def fetch(k):
        for i in range(m):
            j = jnp.where(first, m - 1 - i, i)
            for a, layer, row, rows, col, at in blocks(k):
                there = pl.ds(at, rows)
                remote(
                    deltas[a].at[(0,) + whole_slice(a, layer, row, rows, col, 2 * j + 1 - core)],
                    theirs.at[k, j, there], total_sem.at[0], theirs_sem.at[k, j], partner,
                ).start()
                pltpu.make_async_copy(
                    deltas[a].at[(0,) + whole_slice(a, layer, row, rows, col, 2 * j + core)],
                    mine.at[k, j, there], mine_sem.at[k, j],
                ).start()
        for a, layer, row, rows, col, at in blocks(k):
            there, own = pl.ds(at, rows), own_slice(a, layer, row, rows, col)
            pltpu.make_async_copy(masters[a].at[own], master.at[k, there], state_sem.at[k]).start()
            pltpu.make_async_copy(moments[a].at[own], moment.at[k, there], state_sem.at[k]).start()

    def pair_sum(k, j):
        wait_bytes(theirs.at[k, j], theirs_sem.at[k, j])
        wait_bytes(mine.at[k, j], mine_sem.at[k, j])
        return theirs[k, j].astype(jnp.float32) + mine[k, j].astype(jnp.float32)

    def send_up(k, j):
        remote(mine.at[k, j], up_in.at[k, j], total_sem.at[1], up_sem.at[k, j], above).start()

    def send_down(k, j):
        remote(mine.at[k, j], down_in.at[k, j], total_sem.at[1], down_sem.at[k, j], below).start()

    def begin(k):
        @pl.when(first | last)
        def _():
            for i in range(m - 1):
                j = jnp.where(first, m - 1 - i, i)
                mine[k, j] = pair_sum(k, j).astype(jnp.bfloat16)

                @pl.when(first)
                def _():
                    send_up(k, j)

                @pl.when(last)
                def _():
                    send_down(k, j)

    def forward(s, k):
        up_j = m - 1 + z - s

        @pl.when((z >= 1) & (z <= s) & (z < m - 1))
        def _():
            running = pair_sum(k, up_j)
            wait_bytes(up_in.at[k, up_j], up_sem.at[k, up_j])
            mine[k, up_j] = (running + up_in[k, up_j].astype(jnp.float32)).astype(jnp.bfloat16)
            send_up(k, up_j)

        down_j = s - (m - 1 - z)

        @pl.when((z < m - 1) & (m - 1 - z <= s) & (z >= 1))
        def _():
            running = pair_sum(k, down_j)
            wait_bytes(down_in.at[k, down_j], down_sem.at[k, down_j])
            mine[k, down_j] = (running + down_in[k, down_j].astype(jnp.float32)).astype(jnp.bfloat16)
            send_down(k, down_j)

    def hand_on(k, j, up, down):
        chunk = gathered.at[k, j]

        @pl.when(up)
        def _():
            remote(chunk, chunk, gather_up_sem.at[k, j], gather_sem.at[k, j], above).start()

        @pl.when(down)
        def _():
            remote(chunk, chunk, gather_down_sem.at[k, j], gather_sem.at[k, j], below).start()

        for a, layer, row, rows, col, at in blocks(k):
            source = gathered.at[k, j, pl.ds(at, rows)]
            target = params[a].at[whole_slice(a, layer, row, rows, col, 2 * j + core)]
            remote(source, target, total_sem.at[2], total_sem.at[3], partner).start()
            pltpu.make_async_copy(source, target, total_sem.at[4]).start()

    def update(k):
        total = pair_sum(k, z)
        pltpu.make_async_copy(master.at[k], master.at[k], state_sem.at[k]).wait()
        pltpu.make_async_copy(moment.at[k], moment.at[k], state_sem.at[k]).wait()
        mine_total = total

        def finish(summed):
            average = summed / n
            momentum = OUTER_MOMENTUM * moment[k] + average
            updated = master[k] - OUTER_RATE * (average + OUTER_MOMENTUM * momentum)
            moment[k] = momentum
            master[k] = updated
            gathered[k, z] = updated.astype(jnp.bfloat16)

        @pl.when(z > 0)
        def _():
            wait_bytes(up_in.at[k, z], up_sem.at[k, z])

        @pl.when(z < m - 1)
        def _():
            wait_bytes(down_in.at[k, z], down_sem.at[k, z])

        @pl.when(first)
        def _():
            finish(mine_total + down_in[k, z].astype(jnp.float32))

        @pl.when(last)
        def _():
            finish(mine_total + up_in[k, z].astype(jnp.float32))

        @pl.when(jnp.logical_not(first | last))
        def _():
            finish(mine_total + up_in[k, z].astype(jnp.float32) + down_in[k, z].astype(jnp.float32))

        hand_on(k, z, z < m - 1, z > 0)
        for a, layer, row, rows, col, at in blocks(k):
            there, own = pl.ds(at, rows), own_slice(a, layer, row, rows, col)
            pltpu.make_async_copy(master.at[k, there], new_masters[a].at[own], total_sem.at[5]).start()
            pltpu.make_async_copy(moment.at[k, there], new_moments[a].at[own], total_sem.at[6]).start()

    def gather(g, k):
        low, high = z - g, z + g

        @pl.when(low >= 0)
        def _():
            wait_bytes(gathered.at[k, low], gather_sem.at[k, low])
            hand_on(k, low, z < m - 1, False)

        @pl.when(high < m)
        def _():
            wait_bytes(gathered.at[k, high], gather_sem.at[k, high])
            hand_on(k, high, False, z > 0)

    barrier = pltpu.get_barrier_semaphore()
    pl.semaphore_signal(barrier, inc=1, device_id={"rep": partner}, device_id_type=MESH)

    @pl.when(z > 0)
    def _():
        pl.semaphore_signal(barrier, inc=1, device_id={"rep": below}, device_id_type=MESH)

    @pl.when(z < m - 1)
    def _():
        pl.semaphore_signal(barrier, inc=1, device_id={"rep": above}, device_id_type=MESH)

    pl.semaphore_wait(barrier, 1 + (z > 0).astype(jnp.int32) + (z < m - 1).astype(jnp.int32))

    stages = [begin]
    stages += [functools.partial(forward, s) for s in range(1, m - 1)]
    stages += [update]
    stages += [functools.partial(gather, g) for g in range(1, m)]
    lead = min(LEAD, pieces)

    def early(k, carry):
        fetch(k)
        return carry

    lax.fori_loop(0, lead, early, 0)

    def tick(t, carry):
        @pl.when(t + lead < pieces)
        def _():
            fetch(t + lead)

        for s in reversed(range(len(stages))):
            k = t - s

            @pl.when((k >= 0) & (k < pieces))
            def _():
                stages[s](k)

        return carry

    lax.fori_loop(0, pieces + len(stages) - 1, tick, 0)

    wait_bytes(theirs, total_sem.at[0])
    wait_bytes(theirs.at[:, pl.ds(0, m - 1)], total_sem.at[1])
    for s in range(2, 5):
        wait_bytes(gathered, total_sem.at[s])
    wait_bytes(master, total_sem.at[5])
    wait_bytes(moment, total_sem.at[6])

    def drain(k, carry):
        for j in range(m):
            @pl.when((z < m - 1) & (j <= z))
            def _():
                wait_bytes(gathered.at[k, j], gather_up_sem.at[k, j])

            @pl.when((z > 0) & (j >= z))
            def _():
                wait_bytes(gathered.at[k, j], gather_down_sem.at[k, j])
        return carry

    lax.fori_loop(0, pieces, drain, 0)


def on_device(n, *arrays):
    states = arrays[1::3]
    own_shapes = [x.shape for x in states]
    pieces = PIECES
    while plan(own_shapes, pieces) is None:
        pieces //= 2
    cuts = plan(own_shapes, pieces)
    width = min(cols for _, _, _, cols in cuts)
    while any(cols % width for _, _, _, cols in cuts):
        width -= 128
    depth = sum(rows * (cols // width) for _, _, rows, cols in cuts)
    m = n // 2
    out_shape = []
    for delta, master, moment in zip(arrays[0::3], arrays[1::3], arrays[2::3]):
        out_shape += [
            jax.ShapeDtypeStruct(delta.shape[1:], jnp.bfloat16),
            jax.ShapeDtypeStruct(master.shape, jnp.float32),
            jax.ShapeDtypeStruct(moment.shape, jnp.float32),
        ]
    chunks = pltpu.VMEM((pieces, m, depth, width), jnp.bfloat16)
    state = pltpu.VMEM((pieces, depth, width), jnp.float32)
    flags = pltpu.SemaphoreType.DMA((pieces, m))
    return tuple(
        pl.pallas_call(
            functools.partial(kernel, n, cuts, width, own_shapes),
            out_shape=out_shape,
            in_specs=[pl.BlockSpec(memory_space=pl.ANY)] * len(arrays),
            out_specs=[pl.BlockSpec(memory_space=pl.ANY)] * len(out_shape),
            scratch_shapes=[chunks] * 5 + [state] * 2
            + [flags] * 5 + [pltpu.SemaphoreType.DMA((pieces,))] + [flags] * 2
            + [pltpu.SemaphoreType.DMA((7,))],
            compiler_params=pltpu.CompilerParams(
                collective_id=0, has_side_effects=True, vmem_limit_bytes=60 * 1024 * 1024
            ),
        )(*arrays)
    )


def solution(mesh):
    placed = (
        P("rep", None, None, "tp"),
        P(None, "rep", "tp"),
        P(None, "rep", "tp"),
        P("rep", None, None, "tp"),
        P(None, "rep", "tp"),
        P(None, "rep", "tp"),
        P("rep", None, "tp", None),
        P(None, "tp", "rep"),
        P(None, "tp", "rep"),
    )
    return jax.shard_map(
        functools.partial(on_device, mesh.shape["rep"]),
        mesh=mesh,
        in_specs=placed,
        out_specs=(
            P(None, None, "tp"),
            P(None, "rep", "tp"),
            P(None, "rep", "tp"),
            P(None, None, "tp"),
            P(None, "rep", "tp"),
            P(None, "rep", "tp"),
            P(None, "tp", None),
            P(None, "tp", "rep"),
            P(None, "tp", "rep"),
        ),
        check_vma=False,
    )
```

```python
import functools

import jax
import jax.numpy as jnp
from jax import lax
from jax.experimental import pallas as pl
from jax.experimental.pallas import tpu as pltpu
from jax.sharding import PartitionSpec as P

OUTER_RATE = 0.7
OUTER_MOMENTUM = 0.9
MESH = pl.DeviceIdType.MESH
PIECES = 16
LEAD = 3


def plan(shapes, pieces):
    cuts = []
    for layers, rows, cols in shapes:
        if pieces % layers:
            return None
        per_layer = pieces // layers
        by_row = per_layer
        while by_row > 1 and (rows % by_row or (rows // by_row) % 16):
            by_row //= 2
        by_col = per_layer // by_row
        if by_row * by_col != per_layer or cols % by_col or (cols // by_col) % 128:
            return None
        cuts.append((per_layer, by_col, rows // by_row, cols // by_col))
    return cuts


def kernel(n, cuts, own_shapes, *refs):
    deltas, masters, moments = refs[0:9:3], refs[1:9:3], refs[2:9:3]
    params, new_masters, new_moments = refs[9:18:3], refs[10:18:3], refs[11:18:3]
    theirs, mine, up_in, down_in = refs[18:21], refs[21:24], refs[24:27], refs[27:30]
    (measure, theirs_sem, mine_sem, up_sem, down_sem, gather_sem,
     gather_up_sem, gather_down_sem, total_sem) = refs[30:]
    m = n // 2
    pieces = theirs[0].shape[0]
    me = lax.axis_index("rep")
    z, core = me // 2, me % 2
    partner = z * 2 + 1 - core
    above, below = (z + 1) * 2 + core, (z - 1) * 2 + core
    first, last = z == 0, z == m - 1
    arrays = range(len(cuts))

    def own_slice(a, k):
        per_layer, by_col, rows, cols = cuts[a]
        layer, part = k // per_layer, k % per_layer
        if by_col == 1:
            return (layer, pl.ds(pl.multiple_of(part * rows, 16), rows), pl.ds(0, cols))
        row, col = (part // by_col) * rows, (part % by_col) * cols
        return (layer, pl.ds(pl.multiple_of(row, 16), rows), pl.ds(pl.multiple_of(col, 128), cols))

    def whole_slice(a, k, owner):
        per_layer, by_col, rows, cols = cuts[a]
        layer, part = k // per_layer, k % per_layer
        row, col = (part // by_col) * rows, (part % by_col) * cols
        own_rows, own_cols = own_shapes[a][1:]
        if a < 2:
            row = row + owner * own_rows
        else:
            col = col + owner * own_cols
        if a < 2 and by_col == 1:
            return (layer, pl.ds(pl.multiple_of(row, 16), rows), pl.ds(0, cols))
        return (layer, pl.ds(pl.multiple_of(row, 16), rows), pl.ds(pl.multiple_of(col, 128), cols))

    def remote(src, dst, send, recv, rank):
        return pltpu.make_async_remote_copy(
            src_ref=src, dst_ref=dst, send_sem=send, recv_sem=recv,
            device_id={"rep": rank}, device_id_type=MESH,
        )

    def wait_bytes(ref, sem):
        pltpu.make_async_copy(ref, ref, sem).wait()

    def wait_chunk(sem):
        wait_bytes(measure, sem)

    def fetch(k):
        for i in range(m):
            j = jnp.where(first, m - 1 - i, i)
            for a in arrays:
                remote(
                    deltas[a].at[(0,) + whole_slice(a, k, 2 * j + 1 - core)],
                    theirs[a].at[k, j], total_sem.at[0, a], theirs_sem.at[k, j], partner,
                ).start()
                pltpu.make_async_copy(
                    deltas[a].at[(0,) + whole_slice(a, k, 2 * j + core)],
                    mine[a].at[k, j], mine_sem.at[k, j],
                ).start()

    def wait_pair(k, j):
        wait_chunk(theirs_sem.at[k, j])
        wait_chunk(mine_sem.at[k, j])

    def pair_sum(a, k, j):
        return theirs[a][k, j].astype(jnp.float32) + mine[a][k, j].astype(jnp.float32)

    def send_up(k, j):
        for a in arrays:
            remote(mine[a].at[k, j], up_in[a].at[k, j], total_sem.at[1, a], up_sem.at[k, j], above).start()

    def send_down(k, j):
        for a in arrays:
            remote(mine[a].at[k, j], down_in[a].at[k, j], total_sem.at[1, a], down_sem.at[k, j], below).start()

    def begin(k):
        @pl.when(first | last)
        def _():
            for i in range(m - 1):
                j = jnp.where(first, m - 1 - i, i)
                wait_pair(k, j)
                for a in arrays:
                    mine[a][k, j] = pair_sum(a, k, j).astype(jnp.bfloat16)

                @pl.when(first)
                def _():
                    send_up(k, j)

                @pl.when(last)
                def _():
                    send_down(k, j)

    def forward(s, k):
        up_j = m - 1 + z - s

        @pl.when((z >= 1) & (z <= s) & (z < m - 1))
        def _():
            wait_pair(k, up_j)
            wait_chunk(up_sem.at[k, up_j])
            for a in arrays:
                running = pair_sum(a, k, up_j) + up_in[a][k, up_j].astype(jnp.float32)
                mine[a][k, up_j] = running.astype(jnp.bfloat16)
            send_up(k, up_j)

        down_j = s - (m - 1 - z)

        @pl.when((z < m - 1) & (m - 1 - z <= s) & (z >= 1))
        def _():
            wait_pair(k, down_j)
            wait_chunk(down_sem.at[k, down_j])
            for a in arrays:
                running = pair_sum(a, k, down_j) + down_in[a][k, down_j].astype(jnp.float32)
                mine[a][k, down_j] = running.astype(jnp.bfloat16)
            send_down(k, down_j)

    def hand_on(k, j, up, down):
        chunks = [params[a].at[whole_slice(a, k, 2 * j + core)] for a in arrays]

        @pl.when(up)
        def _():
            for chunk in chunks:
                remote(chunk, chunk, gather_up_sem.at[k, j], gather_sem.at[k, j], above).start()

        @pl.when(down)
        def _():
            for chunk in chunks:
                remote(chunk, chunk, gather_down_sem.at[k, j], gather_sem.at[k, j], below).start()

        for a in arrays:
            remote(chunks[a], chunks[a], total_sem.at[2, a], total_sem.at[3, a], partner).start()

    def update(k):
        wait_pair(k, z)

        @pl.when(k == 0)
        def _():
            for a in arrays:
                wait_bytes(new_masters[a], total_sem.at[4, a])
                wait_bytes(new_moments[a], total_sem.at[5, a])

        @pl.when(z > 0)
        def _():
            wait_chunk(up_sem.at[k, z])

        @pl.when(z < m - 1)
        def _():
            wait_chunk(down_sem.at[k, z])

        def finish(neighbours):
            for a in arrays:
                summed = pair_sum(a, k, z)
                for near in neighbours:
                    summed = summed + near[a][k, z].astype(jnp.float32)
                own = own_slice(a, k)
                average = summed / n
                momentum = OUTER_MOMENTUM * new_moments[a][own] + average
                updated = new_masters[a][own] - OUTER_RATE * (average + OUTER_MOMENTUM * momentum)
                new_moments[a][own] = momentum
                new_masters[a][own] = updated
                params[a][whole_slice(a, k, me)] = updated.astype(jnp.bfloat16)

        @pl.when(first)
        def _():
            finish((down_in,))

        @pl.when(last)
        def _():
            finish((up_in,))

        @pl.when(jnp.logical_not(first | last))
        def _():
            finish((up_in, down_in))

        hand_on(k, z, z < m - 1, z > 0)

    def gather(g, k):
        low, high = z - g, z + g

        @pl.when(low >= 0)
        def _():
            wait_chunk(gather_sem.at[k, low])
            hand_on(k, low, z < m - 1, False)

        @pl.when(high < m)
        def _():
            wait_chunk(gather_sem.at[k, high])
            hand_on(k, high, False, z > 0)

    barrier = pltpu.get_barrier_semaphore()
    pl.semaphore_signal(barrier, inc=1, device_id={"rep": partner}, device_id_type=MESH)

    @pl.when(z > 0)
    def _():
        pl.semaphore_signal(barrier, inc=1, device_id={"rep": below}, device_id_type=MESH)

    @pl.when(z < m - 1)
    def _():
        pl.semaphore_signal(barrier, inc=1, device_id={"rep": above}, device_id_type=MESH)

    pl.semaphore_wait(barrier, 1 + (z > 0).astype(jnp.int32) + (z < m - 1).astype(jnp.int32))

    stages = [begin]
    stages += [functools.partial(forward, s) for s in range(1, m - 1)]
    stages += [update]
    stages += [functools.partial(gather, g) for g in range(1, m)]
    lead = min(LEAD, pieces)

    def early(k, carry):
        fetch(k)
        return carry

    lax.fori_loop(0, lead, early, 0)
    for a in arrays:
        pltpu.make_async_copy(masters[a], new_masters[a], total_sem.at[4, a]).start()
        pltpu.make_async_copy(moments[a], new_moments[a], total_sem.at[5, a]).start()

    def tick(t, carry):
        @pl.when(t + lead < pieces)
        def _():
            fetch(t + lead)

        for s in reversed(range(len(stages))):
            k = t - s

            @pl.when((k >= 0) & (k < pieces))
            def _():
                stages[s](k)

        return carry

    lax.fori_loop(0, pieces + len(stages) - 1, tick, 0)

    for a in arrays:
        wait_bytes(theirs[a], total_sem.at[0, a])
        wait_bytes(theirs[a].at[:, pl.ds(0, m - 1)], total_sem.at[1, a])
        wait_bytes(theirs[a], total_sem.at[2, a])
        wait_bytes(theirs[a], total_sem.at[3, a])

    def drain(k, carry):
        for j in range(m):
            @pl.when((z < m - 1) & (j <= z))
            def _():
                wait_chunk(gather_up_sem.at[k, j])

            @pl.when((z > 0) & (j >= z))
            def _():
                wait_chunk(gather_down_sem.at[k, j])
        return carry

    lax.fori_loop(0, pieces, drain, 0)


def on_device(n, *arrays):
    states = arrays[1::3]
    own_shapes = [x.shape for x in states]
    pieces = PIECES
    while plan(own_shapes, pieces) is None:
        pieces //= 2
    cuts = plan(own_shapes, pieces)
    m = n // 2
    size = sum(rows * cols for _, _, rows, cols in cuts)
    out_shape = []
    for delta, master, moment in zip(arrays[0::3], arrays[1::3], arrays[2::3]):
        out_shape += [
            pltpu.VMEM(delta.shape[1:], jnp.bfloat16),
            pltpu.VMEM(master.shape, jnp.float32),
            pltpu.VMEM(moment.shape, jnp.float32),
        ]
    chunks = [pltpu.VMEM((pieces, m, rows, cols), jnp.bfloat16) for _, _, rows, cols in cuts]
    flags = pltpu.SemaphoreType.DMA((pieces, m))
    scratch_bytes = 4 * 2 * pieces * m * size
    return tuple(
        pl.pallas_call(
            functools.partial(kernel, n, cuts, own_shapes),
            out_shape=out_shape,
            in_specs=[pl.BlockSpec(memory_space=pltpu.HBM)] * len(arrays),
            out_specs=[pl.BlockSpec(memory_space=pltpu.VMEM)] * len(out_shape),
            scratch_shapes=chunks * 4
            + [pltpu.VMEM((size // 128, 128), jnp.bfloat16)]
            + [flags] * 7
            + [pltpu.SemaphoreType.DMA((6, len(cuts)))],
            compiler_params=pltpu.CompilerParams(
                collective_id=0, has_side_effects=True, vmem_limit_bytes=scratch_bytes + 4 * 2**20
            ),
        )(*arrays)
    )


def solution(mesh):
    placed = (
        P("rep", None, None, "tp"),
        P(None, "rep", "tp"),
        P(None, "rep", "tp"),
        P("rep", None, None, "tp"),
        P(None, "rep", "tp"),
        P(None, "rep", "tp"),
        P("rep", None, "tp", None),
        P(None, "tp", "rep"),
        P(None, "tp", "rep"),
    )
    return jax.shard_map(
        functools.partial(on_device, mesh.shape["rep"]),
        mesh=mesh,
        in_specs=placed,
        out_specs=(
            P(None, None, "tp"),
            P(None, "rep", "tp"),
            P(None, "rep", "tp"),
            P(None, None, "tp"),
            P(None, "rep", "tp"),
            P(None, "rep", "tp"),
            P(None, "tp", None),
            P(None, "tp", "rep"),
            P(None, "tp", "rep"),
        ),
        check_vma=False,
    )
```
